32 devices in a mesh: row: 4 (over z), col: 8 (over y, x, core).
Axes of the slice: x: 2, y: 2, z: 4, core: 2. Of those that a mesh axis runs over, the one named last changes fastest.
Arguments:
- tokens: bfloat16 [2048, 2048], P(('row', 'col')), may hold values from -6 to 6
- timestep: int32 [1], replicated, may hold values from 0 to 999
- mod_weight: float32 [256, 2048], replicated, may hold values from -0.375 to 0.375
- qkv_weight: bfloat16 [3, 2048, 2048], P(None, None, 'col'), may hold values from -0.125 to 0.125
- attn_scale: float32 [16], P('col'), may hold values from 4 to 40
- out_weight: bfloat16 [2048, 2048], P('col'), may hold values from -0.5 to 0.5
- grad_update: bfloat16 [2048, 2048], P(('row', 'col')), may hold values from -6 to 6
Outputs:
- update: bfloat16 [2048, 2048], P(('row', 'col'))
- grad_tokens: bfloat16 [2048, 2048], P(('row', 'col'))
- grad_qkv: float32 [3, 2048, 2048], P(None, 'row', 'col')
- grad_out: float32 [2048, 2048], P('col', 'row')
The draws below stay inside these ranges and needn't reach their ends.
All inputs are finite; a program needn't handle non-finite values.
Results may differ from the reference program's by a relative error of at most 0.018.
Values may be sent and summed in bfloat16 or wider, within the bound.
A program may use at most 128 MiB of HBM per device.

```python
import math
import jax
import jax.numpy as jnp
from jax import lax

D = 2048
HEADS = 16
FREQS = 128
HDIM = 128
TOKENS = 2048


def block_levels(key, shape, pieces, least, high):
    def one(position, parts):
        draws = jax.random.uniform(jax.random.fold_in(jax.random.fold_in(key, 6), position), (parts,), jnp.float32, least / len(pieces), high / len(pieces))
        return jnp.repeat(jnp.exp(draws), shape[position] // parts).reshape((-1,) + (1,) * (len(shape) - position - 1))

    loudness = one(*pieces[0])
    for cut in pieces[1:]:
        loudness = loudness * one(*cut)
    return loudness


def centred(stream_key, shape, scale, bound, split=(), held_as=jnp.bfloat16):
    entries = jax.random.normal(stream_key, shape, jnp.float32) * scale
    if len(split) > 0:
        entries = block_levels(stream_key, shape, split, -0.22, 0.18) * entries
    return jnp.clip(entries, min=-bound, max=bound).astype(held_as)


def setup_inputs(seed: int = 0) -> dict:
    streams_of = jax.random.split(jax.random.key(seed), 8)
    tokens = centred(streams_of[0], (TOKENS, D), 1.0, 6.0, ((0, 32),))
    timestep = jax.random.randint(streams_of[1], (1,), 0, 1000).astype(jnp.int32)
    mod_weight = centred(streams_of[2], (2 * FREQS, D), (2 * FREQS) ** -0.5, 0.375, (), jnp.float32)
    qkv_weight = centred(streams_of[3], (3, D, D), D ** -0.5, 0.125, ((2, 8),))
    attn_scale = jnp.clip(jnp.exp(math.log(40.0) - 2.3025851 * jax.random.uniform(streams_of[4], (HEADS,), jnp.float32) ** block_levels(streams_of[4], (HEADS,), ((0, 8),), -0.2, 0.2)), 4.0, 40.0)
    out_weight = centred(streams_of[5], (D, D), HDIM ** -0.5, 0.5, ((0, 8),))
    grad_update = centred(streams_of[6], (TOKENS, D), 1.0, 6.0, ((0, 32),))
    return dict(tokens=tokens, timestep=timestep, mod_weight=mod_weight, qkv_weight=qkv_weight, attn_scale=attn_scale, out_weight=out_weight, grad_update=grad_update)


epsilon = 1e-06

def embed(timestep, count):
    index = jnp.arange(count, dtype=jnp.float32)
    freqs = jnp.exp(-math.log(10000.0) * index / count)
    angles = timestep.astype(jnp.float32)[0] * freqs
    return jnp.concatenate([jnp.cos(angles), jnp.sin(angles)])

def unit_rows(values):
    factor = lax.rsqrt(lax.optimization_barrier(jnp.mean(values * values, -1, keepdims=True)) + epsilon)
    return (values * factor, factor)

def unit_grad(grad_unit, unit, factor):
    return factor * (grad_unit - unit * lax.optimization_barrier(jnp.mean(grad_unit * unit, -1, keepdims=True)))

def forward_head(packed):
    query, key_rows, value_rows, scale = packed
    head_dim = query.shape[1]
    coeff = scale / head_dim
    size = math.gcd(query.shape[0], 512)
    blocks = query.reshape(query.shape[0] // size, size, head_dim)

    def one_block(query_block):
        scores = jnp.dot(query_block, key_rows.T, preferred_element_type=jnp.float32) * coeff
        weights = jnp.exp(scores - scale)
        totals = lax.optimization_barrier(jnp.sum(weights, -1))
        mixed = jnp.dot(weights.astype(jnp.bfloat16), value_rows, preferred_element_type=jnp.float32)
        return (totals, mixed)
    totals, mixed = lax.map(one_block, blocks)
    return (totals.reshape(-1), mixed.reshape(-1, head_dim))

def backward_head(packed):
    query, key_rows, value_rows, grad_rows, delta_rows, inverse_rows, scale = packed
    head_dim = query.shape[1]
    coeff = scale / head_dim
    length = query.shape[0]
    size = math.gcd(length, 512)
    blocks = (query.reshape(length // size, size, head_dim), grad_rows.reshape(length // size, size, head_dim), delta_rows.reshape(length // size, size), inverse_rows.reshape(length // size, size))

    def step(state, block):
        query_block, grad_block, delta_block, inverse_block = block
        scores = jnp.dot(query_block, key_rows.T, preferred_element_type=jnp.float32) * coeff
        probs = jnp.exp(scores - scale) * inverse_block[:, None]
        dprobs = jnp.dot(grad_block, value_rows.T, preferred_element_type=jnp.float32)
        dscores = (probs * (dprobs - delta_block[:, None]) * coeff).astype(jnp.bfloat16)
        grad_query = jnp.dot(dscores, key_rows, preferred_element_type=jnp.float32)
        grad_key = state[0] + jnp.dot(dscores.T, query_block, preferred_element_type=jnp.float32)
        grad_value = state[1] + jnp.dot(probs.astype(jnp.bfloat16).T, grad_block, preferred_element_type=jnp.float32)
        return ((grad_key, grad_value), grad_query)
    empty = jnp.zeros((length, head_dim), jnp.float32)
    (grad_key, grad_value), grad_query = lax.scan(step, (empty, empty), blocks)
    return (grad_query.reshape(length, head_dim), grad_key, grad_value)

def reference(tokens, timestep, mod_weight, qkv_weight, attn_scale, out_weight, grad_update):
    length, width = tokens.shape
    heads = attn_scale.shape[0]
    head_dim = width // heads
    embedded = embed(timestep, mod_weight.shape[0] // 2)
    gain = 1.0 + lax.optimization_barrier(jnp.sum(embedded[:, None] * mod_weight, 0))
    tok_float = tokens.astype(jnp.float32)
    rstd = lax.rsqrt(lax.optimization_barrier(jnp.mean(tok_float * tok_float, -1, keepdims=True)) + epsilon)
    normed = tok_float * rstd
    hidden = (normed * gain).astype(jnp.bfloat16)
    raw = jnp.stack([jnp.dot(hidden, qkv_weight[k], preferred_element_type=jnp.float32) for k in range(3)])
    query_unit, query_factor = unit_rows(raw[0].reshape(length, heads, head_dim))
    key_unit, key_factor = unit_rows(raw[1].reshape(length, heads, head_dim))
    query_heads = jnp.transpose(query_unit.astype(jnp.bfloat16), (1, 0, 2))
    key_heads = jnp.transpose(key_unit.astype(jnp.bfloat16), (1, 0, 2))
    value_heads = jnp.transpose(raw[2].astype(jnp.bfloat16).reshape(length, heads, head_dim), (1, 0, 2))
    totals, mixed = lax.map(forward_head, (query_heads, key_heads, value_heads, attn_scale))
    attended_heads = (mixed / totals[:, :, None]).astype(jnp.bfloat16)
    attended = jnp.transpose(attended_heads, (1, 0, 2)).reshape(length, width)
    update = jnp.dot(attended, out_weight, preferred_element_type=jnp.float32).astype(jnp.bfloat16)
    grad_out = jnp.dot(attended.T, grad_update, preferred_element_type=jnp.float32)
    grad_attended = jnp.dot(grad_update, out_weight.T, preferred_element_type=jnp.float32).astype(jnp.bfloat16)
    grad_heads = jnp.transpose(grad_attended.reshape(length, heads, head_dim), (1, 0, 2))
    delta = lax.optimization_barrier(jnp.sum(grad_heads.astype(jnp.float32) * attended_heads.astype(jnp.float32), -1))
    inverse = 1.0 / totals
    grad_query, grad_key, grad_value = lax.map(backward_head, (query_heads, key_heads, value_heads, grad_heads, delta, inverse, attn_scale))
    grad_query = jnp.transpose(grad_query, (1, 0, 2))
    grad_key = jnp.transpose(grad_key, (1, 0, 2))
    grad_value = jnp.transpose(grad_value, (1, 0, 2))
    grad_q = unit_grad(grad_query, query_unit, query_factor).astype(jnp.bfloat16).reshape(length, width)
    grad_k = unit_grad(grad_key, key_unit, key_factor).astype(jnp.bfloat16).reshape(length, width)
    grad_v = grad_value.astype(jnp.bfloat16).reshape(length, width)
    grad_raw = [grad_q, grad_k, grad_v]
    grad_qkv = jnp.stack([jnp.dot(hidden.T, grad_raw[k], preferred_element_type=jnp.float32) for k in range(3)])
    grad_hidden = jnp.dot(grad_raw[0], qkv_weight[0].T, preferred_element_type=jnp.float32)
    grad_hidden = grad_hidden + jnp.dot(grad_raw[1], qkv_weight[1].T, preferred_element_type=jnp.float32)
    grad_hidden = grad_hidden + jnp.dot(grad_raw[2], qkv_weight[2].T, preferred_element_type=jnp.float32)
    grad_normed = grad_hidden * gain
    grad_tokens = (rstd * (grad_normed - normed * lax.optimization_barrier(jnp.mean(grad_normed * normed, -1, keepdims=True)))).astype(jnp.bfloat16)
    return (update, grad_tokens, grad_qkv, grad_out)
```

```python
import functools
import math

import jax
import jax.numpy as jnp
from jax import lax
from jax.experimental import pallas as pl
from jax.experimental.pallas import tpu as pltpu
from jax.sharding import PartitionSpec as P

epsilon = 1e-06
MESH = pl.DeviceIdType.MESH
RELAYED = 4


def embed(timestep, count):
    index = jnp.arange(count, dtype=jnp.float32)
    freqs = jnp.exp(-math.log(10000.0) * index / count)
    angles = timestep.astype(jnp.float32)[0] * freqs
    return jnp.concatenate([jnp.cos(angles), jnp.sin(angles)])


def by_head(array, head_dim):
    return [array[:, at : at + head_dim] for at in range(0, array.shape[1], head_dim)]


def unit_rows(values):
    factor = lax.rsqrt(jnp.mean(values * values, -1, keepdims=True) + epsilon)
    return (values * factor, factor)


def unit_grad(grad_unit, unit, factor):
    return factor * (grad_unit - unit * jnp.mean(grad_unit * unit, -1, keepdims=True))


def piece(ref, dim, size, index):
    start = index * size
    if dim == len(ref.shape) - 1:
        start = pl.multiple_of(start, 128)
    elif dim == len(ref.shape) - 2:
        start = pl.multiple_of(start, 16)
    return ref.at[(slice(None),) * dim + (pl.ds(start, size),)]


def half(ref, side):
    dim = len(ref.shape) - 2
    size = ref.shape[dim] // 2
    return ref.at[(slice(None),) * dim + (pl.ds(side * size, size),)]


def exchange_kernel(plan, *refs):
    count = len(plan)
    sources, targets = refs[:count], refs[count : 2 * count]
    own_sem, send_sem, recv_sem = refs[2 * count : 2 * count + 3]
    relays = refs[2 * count + 3 :]
    sizes = {axis: n for axis, n, dim, size in plan}
    barrier = pltpu.get_barrier_semaphore()
    for axis, n in sizes.items():
        me = lax.axis_index(axis)
        for step in range(1, n):
            pl.semaphore_signal(
                barrier, inc=1, device_id={axis: lax.rem(me + step, n)}, device_id_type=MESH
            )
    pl.semaphore_wait(barrier, sum(n - 1 for n in sizes.values()))
    def send(job, slot, source, target, peer):
        copy = pltpu.make_async_remote_copy(
            src_ref=source,
            dst_ref=target,
            send_sem=send_sem.at[job, slot],
            recv_sem=recv_sem.at[job, slot],
            device_id={plan[job][0]: peer},
            device_id_type=MESH,
        )
        copy.start()
        return copy

    copies, hops = [], {}
    relayed = [job for job in range(count) if plan[job][1] == RELAYED]
    for job in relayed:
        axis, n, dim, size = plan[job]
        if dim is None:
            continue
        me = lax.axis_index(axis)
        right, left = lax.rem(me + 1, n), lax.rem(me + 3, n)
        opposite = piece(sources[job], dim, size, lax.rem(me + 2, n))
        first = send(job, 4, half(opposite, 0), relays[job].at[0], right)
        second = send(job, 5, half(opposite, 1), relays[job].at[1], left)
        hops[job] = (first, second)
    for step in range(1, max(sizes.values())):
        for job, (axis, n, dim, size) in enumerate(plan):
            if step >= n or (n == RELAYED and step == 2):
                continue
            me = lax.axis_index(axis)
            peer = lax.rem(me + step, n)
            source = sources[job]
            source = source if dim is None else piece(source, dim, size, peer)
            copy = send(job, step, source, targets[job].at[me], peer)
            if n == RELAYED and dim is None:
                hops.setdefault(job, []).append(copy)
            else:
                copies.append(copy)
    for job, (axis, n, dim, size) in enumerate(plan):
        me = lax.axis_index(axis)
        source = sources[job]
        copy = pltpu.make_async_copy(
            source if dim is None else piece(source, dim, size, me),
            targets[job].at[me],
            own_sem.at[job],
        )
        copy.start()
        copies.append(copy)
    for side in range(2):
        for job in relayed:
            axis, n, dim, size = plan[job]
            me = lax.axis_index(axis)
            right, left = lax.rem(me + 1, n), lax.rem(me + 3, n)
            onward, origin = (right, left) if side == 0 else (left, right)
            hops[job][side].wait_recv()
            landing = half(targets[job].at[origin], side)
            source = landing if dim is None else relays[job].at[side]
            copies.append(send(job, 6 + side, source, landing, onward))
    for job in relayed:
        for copy in hops[job]:
            copy.wait_send()
    for copy in copies:
        copy.wait()


def exchange(jobs, collective_id):
    plan, shapes, relays = [], [], []
    for array, axis, dim in jobs:
        n = lax.axis_size(axis)
        block = list(array.shape)
        size = None
        if dim is not None:
            size = block[dim] = block[dim] // n
        plan.append((axis, n, dim, size))
        shapes.append(jax.ShapeDtypeStruct((n,) + tuple(block), array.dtype))
        if n == RELAYED and dim is not None:
            block[-2] //= 2
        else:
            block = [16, 128]
        relays.append(pltpu.VMEM((2,) + tuple(block), array.dtype))
    most = max(2 * RELAYED, max(n for axis, n, dim, size in plan))
    count = len(jobs)
    in_vmem = pl.BlockSpec(memory_space=pltpu.VMEM)
    return pl.pallas_call(
        functools.partial(exchange_kernel, tuple(plan)),
        out_shape=shapes,
        in_specs=[in_vmem] * count,
        out_specs=[in_vmem] * count,
        scratch_shapes=[
            pltpu.SemaphoreType.DMA((count,)),
            pltpu.SemaphoreType.DMA((count, most)),
            pltpu.SemaphoreType.DMA((count, most)),
            *relays,
        ],
        compiler_params=pltpu.CompilerParams(
            collective_id=collective_id, has_side_effects=True, vmem_limit_bytes=48 * 2**20
        ),
        name=f"exchange_{collective_id}",
    )(*[array for array, axis, dim in jobs])


def dot_rows(left, right):
    return lax.dot_general(
        left, right, (((1,), (1,)), ((), ())), preferred_element_type=jnp.float32
    )


def dot_columns(left, right):
    return lax.dot_general(
        left, right, (((0,), (0,)), ((), ())), preferred_element_type=jnp.float32
    )


def attention_kernel(
    scale_ref, q_ref, k_ref, v_ref, g_ref, o_ref, dq_ref, dk_ref, dv_ref, dk_sum, dv_sum
):
    block = pl.program_id(1)
    scale = scale_ref[pl.program_id(0)]
    coeff = scale * (1.0 / q_ref.shape[1])
    query, keys, values, grad = q_ref[...], k_ref[...], v_ref[...], g_ref[...]
    weights = jnp.exp(dot_rows(query, keys) * coeff - scale)
    inverse = 1.0 / jnp.sum(weights, -1, keepdims=True)
    mixed = jnp.dot(weights.astype(jnp.bfloat16), values, preferred_element_type=jnp.float32)
    attended = (mixed * inverse).astype(jnp.bfloat16)
    o_ref[...] = attended
    delta = jnp.sum(
        grad.astype(jnp.float32) * attended.astype(jnp.float32), -1, keepdims=True
    )
    probs = weights * inverse
    dscores = (probs * (dot_rows(grad, values) - delta) * coeff).astype(jnp.bfloat16)
    dq_ref[...] = jnp.dot(dscores, keys, preferred_element_type=jnp.float32)
    dk_part = dot_columns(dscores, query)
    dv_part = dot_columns(probs.astype(jnp.bfloat16), grad)

    @pl.when(block == 0)
    def _():
        dk_sum[...] = dk_part
        dv_sum[...] = dv_part

    @pl.when(block > 0)
    def _():
        dk_sum[...] += dk_part
        dv_sum[...] += dv_part

    @pl.when(block == pl.num_programs(1) - 1)
    def _():
        dk_ref[...] = dk_sum[...].astype(jnp.bfloat16)
        dv_ref[...] = dv_sum[...].astype(jnp.bfloat16)


def attention(attn_scale, queries, keys_values, grads):
    heads = attn_scale.shape[0]
    span, inner = queries.shape
    length = keys_values.shape[0]
    head_dim = inner // heads
    size = math.gcd(span, 256)
    while size * length > 2**19 and size % 32 == 0:
        size //= 2
    mine = pl.BlockSpec((size, head_dim), lambda h, i: (i, h))
    keys = pl.BlockSpec((length, head_dim), lambda h, i: (0, h))
    values = pl.BlockSpec((length, head_dim), lambda h, i: (0, heads + h))
    return pl.pallas_call(
        attention_kernel,
        grid=(heads, span // size),
        out_shape=[
            jax.ShapeDtypeStruct((span, inner), jnp.bfloat16),
            jax.ShapeDtypeStruct((span, inner), jnp.float32),
            jax.ShapeDtypeStruct((length, inner), jnp.bfloat16),
            jax.ShapeDtypeStruct((length, inner), jnp.bfloat16),
        ],
        in_specs=[pl.BlockSpec(memory_space=pltpu.SMEM), mine, keys, values, mine],
        out_specs=[mine, mine, keys, keys],
        scratch_shapes=[pltpu.VMEM((length, head_dim), jnp.float32)] * 2,
        compiler_params=pltpu.CompilerParams(
            dimension_semantics=("arbitrary", "arbitrary"), vmem_limit_bytes=56 * 2**20
        ),
        name="attention",
    )(attn_scale, queries, keys_values, keys_values, grads)


def add_up(slots):
    return jnp.sum(slots.astype(jnp.float32), 0)


def per_device(tokens, timestep, mod_weight, qkv_weight, attn_scale, out_weight, grad_update):
    tok_dev, width = tokens.shape
    heads_here = attn_scale.shape[0]
    inner = qkv_weight.shape[2]
    head_dim = inner // heads_here
    span = tok_dev * lax.axis_size("col")
    embedded = embed(timestep, mod_weight.shape[0] // 2)
    gain = 1.0 + jnp.sum(embedded[:, None] * mod_weight, 0)
    tok_float = tokens.astype(jnp.float32)
    rstd = lax.rsqrt(jnp.mean(tok_float * tok_float, -1, keepdims=True) + epsilon)
    normed = tok_float * rstd
    hidden = (normed * gain).astype(jnp.bfloat16)
    (group,) = exchange([(hidden, "col", None)], 0)
    group = group.reshape(span, width)
    raw = [jnp.dot(group, qkv_weight[k], preferred_element_type=jnp.float32) for k in range(3)]
    query_unit, query_factor = zip(*[unit_rows(part) for part in by_head(raw[0], head_dim)])
    key_unit, key_factor = zip(*[unit_rows(part) for part in by_head(raw[1], head_dim)])
    queries = jnp.concatenate(query_unit, 1).astype(jnp.bfloat16)
    keys_values = jnp.concatenate(key_unit + (raw[2],), 1).astype(jnp.bfloat16)
    all_keys_values, grad_group = exchange(
        [(keys_values, "row", None), (grad_update, "col", None)], 1
    )
    all_keys_values = all_keys_values.reshape(-1, 2 * inner)
    grad_group = grad_group.reshape(span, width)
    grad_attended = dot_rows(grad_group, out_weight).astype(jnp.bfloat16)
    attended, grad_query, key_part, value_part = attention(
        attn_scale, queries, all_keys_values, grad_attended
    )
    update_part = jnp.dot(attended, out_weight, preferred_element_type=jnp.float32).astype(
        jnp.bfloat16
    )
    out_part = dot_columns(attended, grad_group).astype(jnp.bfloat16)
    key_slots, value_slots, update_slots = exchange(
        [(key_part, "row", 0), (value_part, "row", 0), (update_part, "col", 0)], 2
    )
    update = add_up(update_slots).astype(jnp.bfloat16)

    def raw_grads(grad_unit, unit, factor):
        parts = zip(by_head(grad_unit, head_dim), unit, factor)
        return jnp.concatenate([unit_grad(*part) for part in parts], 1).astype(jnp.bfloat16)

    grad_raw = [
        raw_grads(grad_query, query_unit, query_factor),
        raw_grads(add_up(key_slots), key_unit, key_factor),
        add_up(value_slots).astype(jnp.bfloat16),
    ]
    qkv_part = jnp.stack([dot_columns(group, part).astype(jnp.bfloat16) for part in grad_raw])
    hidden_part = (
        sum(dot_rows(part, qkv_weight[k]) for k, part in enumerate(grad_raw))
    ).astype(jnp.bfloat16)
    qkv_slots, hidden_slots, out_slots = exchange(
        [(qkv_part, "row", 1), (hidden_part, "col", 0), (out_part, "row", 1)], 3
    )
    grad_qkv = add_up(qkv_slots)
    grad_out = add_up(out_slots)
    grad_normed = add_up(hidden_slots) * gain
    grad_tokens = (
        rstd * (grad_normed - normed * jnp.mean(grad_normed * normed, -1, keepdims=True))
    ).astype(jnp.bfloat16)
    return (update, grad_tokens, grad_qkv, grad_out)


def solution(mesh):
    placed = (
        P(("row", "col"), None),
        P(),
        P(),
        P(None, None, "col"),
        P("col"),
        P("col", None),
        P(("row", "col"), None),
    )
    return jax.shard_map(
        per_device,
        mesh=mesh,
        in_specs=placed,
        out_specs=(
            P(("row", "col"), None),
            P(("row", "col"), None),
            P(None, "row", "col"),
            P("col", "row"),
        ),
        check_vma=False,
    )
```

```python
import functools
import math

import jax
import jax.numpy as jnp
from jax import lax
from jax.experimental import pallas as pl
from jax.experimental.pallas import tpu as pltpu
from jax.sharding import PartitionSpec as P

epsilon = 1e-06
MESH = pl.DeviceIdType.MESH
RELAYED = 4


def embed(timestep, count):
    index = jnp.arange(count, dtype=jnp.float32)
    freqs = jnp.exp(-math.log(10000.0) * index / count)
    angles = timestep.astype(jnp.float32)[0] * freqs
    return jnp.concatenate([jnp.cos(angles), jnp.sin(angles)])


def by_head(array, head_dim):
    return [array[:, at : at + head_dim] for at in range(0, array.shape[1], head_dim)]


def unit_rows(values):
    factor = lax.rsqrt(jnp.mean(values * values, -1, keepdims=True) + epsilon)
    return (values * factor, factor)


def unit_grad(grad_unit, unit, factor):
    return factor * (grad_unit - unit * jnp.mean(grad_unit * unit, -1, keepdims=True))


def piece(ref, dim, size, index):
    start = index * size
    if isinstance(start, int):
        pass
    elif dim == len(ref.shape) - 1:
        start = pl.multiple_of(start, 128)
    elif dim == len(ref.shape) - 2:
        start = pl.multiple_of(start, 16)
    return ref.at[(slice(None),) * dim + (pl.ds(start, size),)]


def half(ref, side):
    dim = len(ref.shape) - 2
    size = ref.shape[dim] // 2
    return ref.at[(slice(None),) * dim + (pl.ds(side * size, size),)]


def exchange_kernel(plan, *refs):
    count = len(plan)
    sources, targets = refs[:count], refs[count : 2 * count]
    own_sem, send_sem, recv_sem = refs[2 * count : 2 * count + 3]
    relays = refs[2 * count + 3 :]
    sizes = {axis: n for axis, n, dim, size in plan}
    barrier = pltpu.get_barrier_semaphore()
    for axis, n in sizes.items():
        me = lax.axis_index(axis)
        for step in range(1, n):
            pl.semaphore_signal(
                barrier, inc=1, device_id={axis: lax.rem(me + step, n)}, device_id_type=MESH
            )
    pl.semaphore_wait(barrier, sum(n - 1 for n in sizes.values()))
    def send(job, slot, source, target, peer):
        copy = pltpu.make_async_remote_copy(
            src_ref=source,
            dst_ref=target,
            send_sem=send_sem.at[job, slot],
            recv_sem=recv_sem.at[job, slot],
            device_id={plan[job][0]: peer},
            device_id_type=MESH,
        )
        copy.start()
        return copy

    copies, hops = [], {}
    chained = [job for job in range(count) if plan[job][1] == RELAYED and plan[job][2] is not None]
    relayed = [job for job in range(count) if plan[job][1] == RELAYED and job not in chained]
    for step in range(1, max(sizes.values())):
        for job, (axis, n, dim, size) in enumerate(plan):
            if step >= n or job in chained or (n == RELAYED and step == 2):
                continue
            me = lax.axis_index(axis)
            peer = lax.rem(me + step, n)
            source = sources[job]
            source = source if dim is None else piece(source, dim, size, peer)
            copy = send(job, step, source, targets[job].at[me], peer)
            if n == RELAYED and dim is None:
                hops.setdefault(job, []).append(copy)
            else:
                copies.append(copy)
    for job, (axis, n, dim, size) in enumerate(plan):
        if job in chained:
            continue
        me = lax.axis_index(axis)
        source = sources[job]
        copy = pltpu.make_async_copy(
            source if dim is None else piece(source, dim, size, me),
            targets[job].at[me],
            own_sem.at[job],
        )
        copy.start()
        copies.append(copy)
    for side in range(2):
        for job in relayed:
            axis, n, dim, size = plan[job]
            me = lax.axis_index(axis)
            right, left = lax.rem(me + 1, n), lax.rem(me + 3, n)
            onward, origin = (right, left) if side == 0 else (left, right)
            hops[job][side].wait_recv()
            landing = half(targets[job].at[origin], side)
            copies.append(send(job, 6 + side, landing, landing, onward))
    def link(job, way, owner, source):
        axis = plan[job][0]
        me = lax.axis_index(axis)
        slot = owner - 1 if way == 0 else owner
        return pltpu.make_async_remote_copy(
            src_ref=relays[job].at[way, slot] if source is None else source,
            dst_ref=relays[job].at[way, slot],
            send_sem=send_sem.at[job, 3 * way + slot],
            recv_sem=recv_sem.at[job, 3 * way + slot],
            device_id={axis: lax.rem(me + (1 if way == 0 else RELAYED - 1), RELAYED)},
            device_id_type=MESH,
        )

    def forward(job, way, owner, place):
        axis, n, dim, size = plan[job]
        mine = piece(sources[job], dim, size, owner)

        @pl.when(lax.axis_index(axis) == place)
        def _():
            if place == (0 if way == 0 else n - 1):
                link(job, way, owner, mine).start()
            else:
                copy = link(job, way, owner, None)
                copy.wait_recv()
                inbox = relays[job].at[way, owner - 1 if way == 0 else owner]
                total = inbox[...].astype(jnp.float32) + mine[...].astype(jnp.float32)
                inbox[...] = total.astype(inbox.dtype)
                copy.start()

    order = [(0, 3, 0), (1, 0, 3), (0, 2, 0), (1, 1, 3), (0, 1, 0), (1, 2, 3)]
    order += [(0, 3, 1), (1, 0, 2), (0, 2, 1), (1, 1, 2), (0, 3, 2), (1, 0, 1)]
    for way, owner, place in order:
        for job in chained:
            forward(job, way, owner, place)
    for job in chained:
        axis, n, dim, size = plan[job]
        for owner in range(n):

            @pl.when(lax.axis_index(axis) == owner)
            def _():
                total = piece(sources[job], dim, size, owner)[...].astype(jnp.float32)
                if owner > 0:
                    link(job, 0, owner, None).wait_recv()
                    total = total + relays[job][0, owner - 1].astype(jnp.float32)
                if owner < n - 1:
                    link(job, 1, owner, None).wait_recv()
                    total = total + relays[job][1, owner].astype(jnp.float32)
                targets[job][0] = total
                for other in range(n):
                    if other > owner:
                        link(job, 0, other, None).wait_send()
                    if other < owner:
                        link(job, 1, other, None).wait_send()

    for job in relayed:
        for copy in hops[job]:
            copy.wait_send()
    for copy in copies:
        copy.wait()


def exchange(jobs, collective_id):
    plan, shapes, relays = [], [], []
    for array, axis, dim in jobs:
        n = lax.axis_size(axis)
        block = list(array.shape)
        size = None
        if dim is not None:
            size = block[dim] = block[dim] // n
        plan.append((axis, n, dim, size))
        if n == RELAYED and dim is not None:
            shapes.append(jax.ShapeDtypeStruct((1,) + tuple(block), jnp.float32))
            relays.append(pltpu.VMEM((2, n - 1) + tuple(block), array.dtype))
        else:
            shapes.append(jax.ShapeDtypeStruct((n,) + tuple(block), array.dtype))
            relays.append(pltpu.VMEM((16, 128), array.dtype))
    most = max(2 * RELAYED, max(n for axis, n, dim, size in plan))
    count = len(jobs)
    in_vmem = pl.BlockSpec(memory_space=pltpu.VMEM)
    return pl.pallas_call(
        functools.partial(exchange_kernel, tuple(plan)),
        out_shape=shapes,
        in_specs=[in_vmem] * count,
        out_specs=[in_vmem] * count,
        scratch_shapes=[
            pltpu.SemaphoreType.DMA((count,)),
            pltpu.SemaphoreType.DMA((count, most)),
            pltpu.SemaphoreType.DMA((count, most)),
            *relays,
        ],
        compiler_params=pltpu.CompilerParams(
            collective_id=collective_id, has_side_effects=True, vmem_limit_bytes=48 * 2**20
        ),
        name=f"exchange_{collective_id}",
    )(*[array for array, axis, dim in jobs])


def dot_rows(left, right):
    return lax.dot_general(
        left, right, (((1,), (1,)), ((), ())), preferred_element_type=jnp.float32
    )


def dot_columns(left, right):
    return lax.dot_general(
        left, right, (((0,), (0,)), ((), ())), preferred_element_type=jnp.float32
    )


def attention_kernel(
    scale_ref, q_ref, k_ref, v_ref, g_ref, o_ref, dq_ref, dk_ref, dv_ref, dk_sum, dv_sum
):
    block = pl.program_id(1)
    scale = scale_ref[pl.program_id(0)]
    coeff = scale * (1.0 / q_ref.shape[1])
    query, keys, values, grad = q_ref[...], k_ref[...], v_ref[...], g_ref[...]
    weights = jnp.exp(dot_rows(query, keys) * coeff - scale)
    inverse = 1.0 / jnp.sum(weights, -1, keepdims=True)
    mixed = jnp.dot(weights.astype(jnp.bfloat16), values, preferred_element_type=jnp.float32)
    attended = (mixed * inverse).astype(jnp.bfloat16)
    o_ref[...] = attended
    delta = jnp.sum(
        grad.astype(jnp.float32) * attended.astype(jnp.float32), -1, keepdims=True
    )
    probs = weights * inverse
    dscores = (probs * (dot_rows(grad, values) - delta) * coeff).astype(jnp.bfloat16)
    dq_ref[...] = jnp.dot(dscores, keys, preferred_element_type=jnp.float32)
    dk_part = dot_columns(dscores, query)
    dv_part = dot_columns(probs.astype(jnp.bfloat16), grad)

    @pl.when(block == 0)
    def _():
        dk_sum[...] = dk_part
        dv_sum[...] = dv_part

    @pl.when(block > 0)
    def _():
        dk_sum[...] += dk_part
        dv_sum[...] += dv_part

    @pl.when(block == pl.num_programs(1) - 1)
    def _():
        dk_ref[...] = dk_sum[...].astype(jnp.bfloat16)
        dv_ref[...] = dv_sum[...].astype(jnp.bfloat16)


def attention(attn_scale, queries, keys_values, grads):
    heads = attn_scale.shape[0]
    span, inner = queries.shape
    length = keys_values.shape[0]
    head_dim = inner // heads
    size = math.gcd(span, 256)
    while size * length > 2**19 and size % 32 == 0:
        size //= 2
    mine = pl.BlockSpec((size, head_dim), lambda h, i: (i, h))
    keys = pl.BlockSpec((length, head_dim), lambda h, i: (0, h))
    values = pl.BlockSpec((length, head_dim), lambda h, i: (0, heads + h))
    return pl.pallas_call(
        attention_kernel,
        grid=(heads, span // size),
        out_shape=[
            jax.ShapeDtypeStruct((span, inner), jnp.bfloat16),
            jax.ShapeDtypeStruct((span, inner), jnp.float32),
            jax.ShapeDtypeStruct((length, inner), jnp.bfloat16),
            jax.ShapeDtypeStruct((length, inner), jnp.bfloat16),
        ],
        in_specs=[pl.BlockSpec(memory_space=pltpu.SMEM), mine, keys, values, mine],
        out_specs=[mine, mine, keys, keys],
        scratch_shapes=[pltpu.VMEM((length, head_dim), jnp.float32)] * 2,
        compiler_params=pltpu.CompilerParams(
            dimension_semantics=("arbitrary", "arbitrary"), vmem_limit_bytes=56 * 2**20
        ),
        name="attention",
    )(attn_scale, queries, keys_values, keys_values, grads)


def add_up(slots):
    return jnp.sum(slots.astype(jnp.float32), 0)


def per_device(tokens, timestep, mod_weight, qkv_weight, attn_scale, out_weight, grad_update):
    tok_dev, width = tokens.shape
    heads_here = attn_scale.shape[0]
    inner = qkv_weight.shape[2]
    head_dim = inner // heads_here
    span = tok_dev * lax.axis_size("col")
    embedded = embed(timestep, mod_weight.shape[0] // 2)
    gain = 1.0 + jnp.sum(embedded[:, None] * mod_weight, 0)
    tok_float = tokens.astype(jnp.float32)
    rstd = lax.rsqrt(jnp.mean(tok_float * tok_float, -1, keepdims=True) + epsilon)
    normed = tok_float * rstd
    hidden = (normed * gain).astype(jnp.bfloat16)
    (group,) = exchange([(hidden, "col", None)], 0)
    group = group.reshape(span, width)
    raw = [jnp.dot(group, qkv_weight[k], preferred_element_type=jnp.float32) for k in range(3)]
    query_unit, query_factor = zip(*[unit_rows(part) for part in by_head(raw[0], head_dim)])
    key_unit, key_factor = zip(*[unit_rows(part) for part in by_head(raw[1], head_dim)])
    queries = jnp.concatenate(query_unit, 1).astype(jnp.bfloat16)
    keys_values = jnp.concatenate(key_unit + (raw[2],), 1).astype(jnp.bfloat16)
    all_keys_values, grad_group = exchange(
        [(keys_values, "row", None), (grad_update, "col", None)], 1
    )
    all_keys_values = all_keys_values.reshape(-1, 2 * inner)
    grad_group = grad_group.reshape(span, width)
    grad_attended = dot_rows(grad_group, out_weight).astype(jnp.bfloat16)
    attended, grad_query, key_part, value_part = attention(
        attn_scale, queries, all_keys_values, grad_attended
    )
    update_part = jnp.dot(attended, out_weight, preferred_element_type=jnp.float32).astype(
        jnp.bfloat16
    )
    out_part = dot_columns(attended, grad_group).astype(jnp.bfloat16)
    key_slots, value_slots, update_slots = exchange(
        [(key_part, "row", 0), (value_part, "row", 0), (update_part, "col", 0)], 2
    )
    update = add_up(update_slots).astype(jnp.bfloat16)

    def raw_grads(grad_unit, unit, factor):
        parts = zip(by_head(grad_unit, head_dim), unit, factor)
        return jnp.concatenate([unit_grad(*part) for part in parts], 1).astype(jnp.bfloat16)

    grad_raw = [
        raw_grads(grad_query, query_unit, query_factor),
        raw_grads(add_up(key_slots), key_unit, key_factor),
        add_up(value_slots).astype(jnp.bfloat16),
    ]
    qkv_part = jnp.stack([dot_columns(group, part).astype(jnp.bfloat16) for part in grad_raw])
    hidden_part = (
        sum(dot_rows(part, qkv_weight[k]) for k, part in enumerate(grad_raw))
    ).astype(jnp.bfloat16)
    qkv_slots, hidden_slots, out_slots = exchange(
        [(qkv_part, "row", 1), (hidden_part, "col", 0), (out_part, "row", 1)], 3
    )
    grad_qkv = add_up(qkv_slots)
    grad_out = add_up(out_slots)
    grad_normed = add_up(hidden_slots) * gain
    grad_tokens = (
        rstd * (grad_normed - normed * jnp.mean(grad_normed * normed, -1, keepdims=True))
    ).astype(jnp.bfloat16)
    return (update, grad_tokens, grad_qkv, grad_out)


def solution(mesh):
    placed = (
        P(("row", "col"), None),
        P(),
        P(),
        P(None, None, "col"),
        P("col"),
        P("col", None),
        P(("row", "col"), None),
    )
    return jax.shard_map(
        per_device,
        mesh=mesh,
        in_specs=placed,
        out_specs=(
            P(("row", "col"), None),
            P(("row", "col"), None),
            P(None, "row", "col"),
            P("col", "row"),
        ),
        check_vma=False,
    )
```
